128 devices in a mesh: gx: 8 (over x, z_hi), gy: 16 (over y, z_lo, core).
Axes of the slice: x: 4, y: 4, z: 4 (z_hi: 2, z_lo: 2; z = z_hi * 2 + z_lo), core: 2. Of those that a mesh axis runs over, the one named last changes fastest.
Arguments:
- traveltime: float32 [8, 32, 128, 1024], P(None, None, 'gy', 'gx'), may hold values from 1 to 4
- adjoint_start: float32 [8, 32, 128, 1024], P(None, None, 'gy', 'gx'), may hold values from -6 to 6
- upwind_flags: int32 [8, 32, 128, 1024], P(None, None, 'gy', 'gx'), may hold values from 0 to 7, as said below
- slowness: float32 [32, 128, 1024], P(None, 'gy', 'gx'), may hold values from 0.15 to 0.6
- residual_rows: float32 [32768, 8], P(('gx', 'gy')), may hold values from -6 to 6
- station_tile: int32 [32768, 1], P(('gx', 'gy')), may hold values from 0 to 127; in each aligned block of 256 rows (0 to 255, 256 to 511, ...) at most 4 rows name the same one
- station_cell: int32 [32768], P(('gx', 'gy')), may hold values from 0 to 32767
Outputs:
- adjoint: float32 [8, 32, 128, 1024], P(None, None, 'gy', 'gx')
- gradient: float32 [32, 128, 1024], P(None, 'gy', 'gx')
The draws below stay inside these ranges and needn't reach their ends.
Inputs may be any that keep to these rules, and one draw needn't show every extreme that they name: `upwind_flags`: bit k of a cell's value is 1 where its upwind neighbour along x, y, z (k = 0, 1, 2) lies at the higher index; at every face of the grid the upwind neighbour lies inside the grid. `station_tile`: among the records of one device no tile is named more than 4 times, a bound that some block reaches.
All inputs are finite; a program needn't handle non-finite values.
Results may differ from the reference program's by a relative error of at most 0.00002.
Values sent between devices are 32-bit elements; how exact they have to be, the bound alone decides.
No kernel may reach another device: no remote copies, remote signals or barrier semaphores. Data moves between devices by JAX's collectives and lax.ppermute only.
A program may use at most 128 MiB of HBM per device.

```python
import math
import jax
import jax.numpy as jnp
import numpy as np
from jax import lax

S = 8
Z = 32
TY = 8
TX = 128
SWEEPS = 3
CAP = 4
ST_DEV = 256
STATIONS = 32768
NX = 1024
NY = 128
N_GY = 16
DEVICES = 128


def draw_upwind_flags(key, part):
    shape = (S, Z, NY, NX)
    bits = jax.random.randint(key, shape, 0, 8)
    along_x = bits % 2
    along_y = bits // 2 % 2
    along_z = bits // 4
    place_x = lax.broadcasted_iota(jnp.int32, shape, 3)
    place_y = lax.broadcasted_iota(jnp.int32, shape, 2)
    place_z = lax.broadcasted_iota(jnp.int32, shape, 1)
    along_x = jnp.where(place_x == 0, 1, jnp.where(place_x == NX - 1, 0, along_x))
    along_y = jnp.where(place_y == 0, 1, jnp.where(place_y == NY - 1, 0, along_y))
    along_z = jnp.where(place_z == 0, 1, jnp.where(place_z == Z - 1, 0, along_z))
    return (along_x + 2 * along_y + 4 * along_z).astype(jnp.int32)


def with_ends(result, own_key, low, top_value):
    spot = [jax.random.randint(jax.random.fold_in(own_key, axis), (), 0, length) for axis, length in enumerate(result.shape)]
    main_axis = result.shape.index(max(result.shape))
    neighbour = spot[:main_axis] + [(spot[main_axis] + 1) % result.shape[main_axis]] + spot[main_axis + 1:]
    return result.at[tuple(spot)].set(low).at[tuple(neighbour)].set(top_value)


def steps_of(own_key, extent, pieces, least, top_value):
    def one(axis_at, blocks):
        steps = jax.random.uniform(jax.random.fold_in(jax.random.fold_in(own_key, 6), axis_at), (blocks,), jnp.float32, least / len(pieces), top_value / len(pieces))
        return jnp.repeat(jnp.exp(steps), extent[axis_at] // blocks).reshape((-1,) + (1,) * (len(extent) - axis_at - 1))

    loudness = one(*pieces[0])
    for cut in pieces[1:]:
        loudness = loudness * one(*cut)
    return loudness


def shared_out(own_key, own, number, rows, amount, top, most, slope):
    order = jax.random.permutation(own_key, amount)
    crowded, usual = shares(amount, rows * top, most, slope, True), shares(amount, rows * top, most, slope, False)
    places = jnp.arange(amount)

    def named(sizes, turn):
        used = int((sizes > 0).sum())
        fixed = max(1, used // 4)
        moved = fixed + (places - fixed + turn * (used - fixed)) % max(1, amount - fixed)
        return jnp.zeros((amount,), jnp.int32).at[order[jnp.where(places < fixed, places, moved)]].set(jnp.asarray(sizes, jnp.int32))

    sizes = jnp.where(number % 4 == 0, named(crowded, number // 4), named(usual, number - number // 4 - 1))
    mixed = jax.random.permutation(jax.random.fold_in(own, 3), amount)
    donor, taker = mixed[0:amount // 2 * 2:2], mixed[1:amount // 2 * 2:2]
    slack = jnp.minimum(sizes[donor] - 1, most - sizes[taker]) // 2
    slack = jnp.where((donor == order[0]) | (taker == order[0]) | (sizes[taker] == 0), 0, jnp.maximum(slack, 0))
    moved = jax.random.randint(jax.random.fold_in(own, 4), (amount // 2,), 0, 1 << 20) % (slack + 1)
    sizes = sizes.at[donor].add(-moved).at[taker].add(moved)
    members = jnp.searchsorted(jnp.cumsum(sizes), jnp.arange(rows * top), side="right").astype(jnp.int32)
    grid = members.reshape(top, rows).T
    grid = grid[jax.random.permutation(jax.random.fold_in(own, 1), rows)]
    turn = jax.random.randint(jax.random.fold_in(own, 2), (rows, 1), 0, top)
    return jnp.take_along_axis(grid, (jnp.arange(top)[None, :] + turn) % top, axis=1)


def shares(count, total, most, skew, full):
    portions = [(1 << 20) // math.isqrt(rank ** skew) + 1 for rank in range(1, count + 1)]
    largest = most if full else min(most, max(-(-total // count), total * portions[0] // sum(portions)))
    least = 1 if total - largest >= count - 1 else 0
    given, surplus = [largest] + [least] * (count - 1), total - largest - least * (count - 1)
    while surplus > 0:
        movable = [i for i in range(1, count) if given[i] < largest] or [i for i in range(1, count) if given[i] < most]
        pool, budget = sum([portions[i] for i in movable]), surplus
        for i in movable:
            more = min(most - given[i], max(1, budget * portions[i] // pool), surplus)
            given[i] = given[i] + more
            surplus = surplus - more
    return np.array(given)


def normal_values(own_key, dims, width, most, pieces=(), kind=jnp.bfloat16):
    drawn = width * jax.random.normal(own_key, dims, jnp.float32)
    if pieces:
        drawn = drawn * steps_of(own_key, dims, pieces, -0.22, 0.18)
    return jnp.clip(drawn, -most, most).astype(kind)


def setup_inputs(seed: int = 0) -> dict:
    key_of = jax.random.split(jax.random.key(seed), 8)
    traveltime = jnp.clip(1.0 + 3.0 * jax.random.uniform(key_of[0], (S, Z, NY, NX), jnp.float32) ** steps_of(key_of[0], (S, Z, NY, NX), ((2, 16), (3, 8)), -0.2, 0.2), 1.0, 4.0)
    adjoint_start = normal_values(key_of[1], (S, Z, NY, NX), 1.0, 6.0, ((2, 16), (3, 8)), jnp.float32)
    upwind_flags = draw_upwind_flags(jax.random.fold_in(key_of[7], 71), 0)
    slowness = jnp.clip(jnp.exp(math.log(0.6) - 1.3862944 * jax.random.uniform(key_of[3], (Z, NY, NX), jnp.float32) ** steps_of(key_of[3], (Z, NY, NX), ((1, 16), (2, 8)), -0.2, 0.2)), 0.15, 0.6)
    residual_rows = normal_values(key_of[4], (STATIONS, S), 1.0, 6.0, ((0, 128),), jnp.float32)
    station_tile_keys = jax.random.split(jax.random.fold_in(key_of[5], 1), STATIONS // ST_DEV)
    station_tile_turns = jax.random.permutation(jax.random.fold_in(key_of[5], 3), STATIONS // ST_DEV)
    station_tile = jax.vmap(lambda own, number: shared_out(jax.random.fold_in(key_of[5], 2), own, number, ST_DEV, DEVICES, 1, CAP, 1))(station_tile_keys, station_tile_turns).reshape((STATIONS, 1))
    station_cell = with_ends(jax.random.randint(key_of[6], (STATIONS,), 0, Z * TY * TX), jax.random.fold_in(key_of[6], 1), 0, (Z * TY * TX) - 1).astype(jnp.int32)
    return {"traveltime": traveltime, "adjoint_start": adjoint_start, "upwind_flags": upwind_flags, "slowness": slowness, "residual_rows": residual_rows, "station_tile": station_tile, "station_cell": station_cell}


def hpad(values):
    widths = [(0, 0)] * (values.ndim - 2) + [(1, 1), (1, 1)]
    return jnp.pad(values, widths)


def relax(adjoint, push_x, push_y, push_z, source, denominator):
    plus_x = jnp.maximum(push_x, 0.0) * adjoint
    minus_x = jnp.maximum(-push_x, 0.0) * adjoint
    plus_y = jnp.maximum(push_y, 0.0) * adjoint
    minus_y = jnp.maximum(-push_y, 0.0) * adjoint
    plus_z = jnp.pad(jnp.maximum(push_z, 0.0) * adjoint, ((0, 0), (1, 1), (0, 0), (0, 0)))
    minus_z = jnp.pad(jnp.maximum(-push_z, 0.0) * adjoint, ((0, 0), (1, 1), (0, 0), (0, 0)))
    inflow = plus_x[:, :, 1:-1, :-2] + minus_x[:, :, 1:-1, 2:] + plus_y[:, :, :-2, 1:-1] + minus_y[:, :, 2:, 1:-1]
    vertical = plus_z[:, :-2] + minus_z[:, 2:]
    inflow = inflow + vertical[:, :, 1:-1, 1:-1]
    return (source[:, :, 1:-1, 1:-1] + inflow) / denominator[:, :, 1:-1, 1:-1]


def smooth(extended):
    centre = extended[:, 1:-1, 1:-1]
    beside = extended[:, 1:-1, 2:] + extended[:, 1:-1, :-2] + extended[:, 2:, 1:-1] + extended[:, :-2, 1:-1]
    return centre + 0.125 * (beside - 4.0 * centre)


def reference(traveltime, adjoint_start, upwind_flags, slowness, residual_rows, station_tile, station_cell):
    sources, levels, rows_y, rows_x = traveltime.shape
    tiles = station_tile[:, 0]
    tile_x = tiles // N_GY
    tile_y = tiles % N_GY
    level = station_cell // (TY * TX)
    cell_y = tile_y * TY + (station_cell // TX) % TY
    cell_x = tile_x * TX + station_cell % TX
    flat = ((level * rows_y + cell_y) * rows_x + cell_x).astype(jnp.int32)
    source = jnp.zeros((sources, levels * rows_y * rows_x), jnp.float32)
    source = source.at[:, flat].add(residual_rows.T).reshape(sources, levels, rows_y, rows_x)
    padded = jnp.pad(traveltime, ((0, 0), (1, 1), (1, 1), (1, 1)))
    plus_x = (upwind_flags % 2) == 1
    plus_y = ((upwind_flags // 2) % 2) == 1
    plus_z = (upwind_flags // 4) == 1
    up_x = jnp.where(plus_x, padded[:, 1:-1, 1:-1, 2:], padded[:, 1:-1, 1:-1, :-2])
    up_y = jnp.where(plus_y, padded[:, 1:-1, 2:, 1:-1], padded[:, 1:-1, :-2, 1:-1])
    up_z = jnp.where(plus_z, padded[:, 2:, 1:-1, 1:-1], padded[:, :-2, 1:-1, 1:-1])
    coef_x = jnp.maximum(traveltime - up_x, 0.0)
    coef_y = jnp.maximum(traveltime - up_y, 0.0)
    coef_z = jnp.maximum(traveltime - up_z, 0.0)
    push_x = jnp.where(plus_x, coef_x, -coef_x)
    push_y = jnp.where(plus_y, coef_y, -coef_y)
    push_z = jnp.where(plus_z, coef_z, -coef_z)
    denominator = 1.0 + coef_x + coef_y + coef_z
    adjoint = adjoint_start
    for repeat in range(SWEEPS):
        adjoint = relax(hpad(adjoint), hpad(push_x), hpad(push_y), hpad(push_z), hpad(source), hpad(denominator))
    total = jnp.sum(adjoint, axis=0)
    gradient = slowness * smooth(hpad(total))
    return adjoint, gradient
```

```python
import jax
import jax.numpy as jnp
from jax import lax
from jax.experimental import pallas as pl
from jax.experimental.pallas import tpu as pltpu
from jax.sharding import PartitionSpec as P

F32 = jnp.float32
BF16 = jnp.bfloat16
I32 = jnp.int32

SRC = 8
Z = 32
TY = 8
TX = 128
PLANES = SRC + 1
ROWS = Z * TY
HALO = 4
CAP = 4
GROUP = 40
PAD = 8
NEAR = tuple((dx, dy) for dx in (-1, 0, 1) for dy in (-1, 0, 1))

NT = (((1,), (1,)), ((), ()))
NN = (((1,), (0,)), ((), ()))


def iota(shape, dim):
    return lax.broadcasted_iota(I32, shape, dim)


def turn(v, by):
    return pltpu.roll(v, by % TX, 1)


def level(z):
    return pl.ds(pl.multiple_of(z * TY, TY), TY)


def dot(a, b, dims=NT):
    return lax.dot_general(a, b, dims, preferred_element_type=F32)


def split3(v):
    hi = v.astype(BF16).astype(F32)
    rest = v - hi
    mid = rest.astype(BF16).astype(F32)
    return hi, mid, rest - mid


def is_even(axis):
    return lax.rem(lax.axis_index(axis), 2) == 0


def records_kernel(rows_ref, tile_ref, cell_ref, out_ref, parts, shifted):
    count = rows_ref.shape[1]
    devices = out_ref.shape[0]
    tile = tile_ref[...]
    named = (iota((devices, count), 0) == tile).astype(F32)
    earlier = (iota((count, count), 0) < iota((count, count), 1)).astype(F32).astype(BF16)
    picks = named.astype(BF16)
    before = dot(picks, earlier, NN)
    rank = jnp.sum(before * named, axis=0, keepdims=True).astype(I32)
    values = rows_ref[...]
    cells = (cell_ref[...] + 1).astype(F32)
    blocks = [jnp.where(rank == k, values, 0.0) for k in range(CAP)]
    blocks.append(jnp.where(rank == iota((8, count), 0), cells, 0.0))
    for k, block in enumerate(blocks):
        for n, part in enumerate(split3(block)):
            parts[n, 8 * k : 8 * k + 8, :] = part
    own = sum(dot(picks, parts[n].astype(BF16)) for n in range(3))
    shifted[...] = jnp.zeros(shifted.shape, F32)
    shifted[32 : 32 + devices, 0:GROUP] = own
    lane = iota((devices, TX), 1)
    ty = lax.rem(iota((devices, TX), 0), 16)
    for c in range(3):
        chunk = jnp.zeros((devices, TX), F32)
        for i in range(3):
            dx, dy = NEAR[3 * c + i]
            off = 32 + 16 * dx + dy
            theirs = shifted[off : off + devices, :]
            held = (lane >= GROUP * i) & (lane < GROUP * (i + 1))
            if dy:
                held = held & (ty + dy >= 0) & (ty + dy < 16)
            chunk = jnp.where(held, turn(theirs, GROUP * i) if i else theirs, chunk)
        out_ref[:, c * TX : (c + 1) * TX] = chunk


def edges_kernel(t_ref, a_ref, f_ref, first_ref, second_ref, own_ref):
    even = is_even("gx")
    lane = iota((TY, TX), 1)
    j = lane & 7

    def at_level(z, carry):
        here = level(z)
        packed = []
        for n, ref in enumerate((t_ref, a_ref, f_ref)):
            both = None
            for s in range(SRC):
                v = turn(ref[s, here, :].astype(F32), HALO + 8 * s)
                both = v if both is None else jnp.where(lane >> 3 == s, v, both)
            own_ref[n, here, :] = both
            packed.append(both)
        t, a, f = packed
        f = turn(f, 64)
        to_right = jnp.where(lane < 64, jnp.where(j < 4, t, turn(a, 4)), f)
        to_left = jnp.where(lane < 64, jnp.where(j < 4, turn(t, -4), a), f)
        first_ref[here, :] = jnp.where(even, to_right, to_left)
        second_ref[here, :] = jnp.where(even, to_left, to_right)
        return carry

    lax.fori_loop(0, Z, at_level, 0, unroll=2)


def strips_kernel(
    t_ref, a_ref, f_ref, own_ref, x0_ref, x1_ref, strip_ref, first_ref, second_ref
):
    even = is_even("gx")
    lane = iota((TY, TX), 1)
    j = lane & 7
    near = j < 4

    def at_level(z, carry):
        here = level(z)
        x0, x1 = x0_ref[here, :], x1_ref[here, :]
        left = jnp.where(even, x1, x0)
        right = jnp.where(even, x0, x1)
        t, a, f = own_ref[0, here, :], own_ref[1, here, :], own_ref[2, here, :]
        strip_ref[0, here, :] = jnp.where(
            lane < 64,
            jnp.where(near, left, t),
            turn(jnp.where(near, t, turn(right, 4)), 64),
        )
        strip_ref[1, here, :] = jnp.where(
            lane < 64,
            jnp.where(near, turn(left, -4), a),
            turn(jnp.where(near, a, right), 64),
        )
        strip_ref[2, here, :] = jnp.where(
            lane < 64,
            jnp.where(near, turn(left, 64), f),
            jnp.where(near, turn(f, 64), right),
        )
        return carry

    lax.fori_loop(0, Z, at_level, 0, unroll=2)

    def pack(out, high):
        edge = pl.ds(TY - 1 if high else 0, Z, stride=TY)
        inner = pl.ds(TY - 2 if high else 1, Z, stride=TY)
        for p in range(PLANES):
            if p < SRC:
                t, a, f = t_ref.at[p], a_ref.at[p], f_ref.at[p]
            else:
                t, a, f = strip_ref.at[0], strip_ref.at[1], strip_ref.at[2]
            out[0, p] = t[edge, :]
            out[1, p] = f[edge, :].astype(F32)
            out[2, p] = a[edge, :]
            out[3, p] = t[inner, :]
            up = (f[inner, :].astype(I32) & 2) != 0
            given = a[inner, :]
            out[4, p] = jnp.where(up, given, 0.0) if high else jnp.where(up, 0.0, given)

    even_y = is_even("gy")

    @pl.when(even_y)
    def _():
        pack(first_ref, True)
        pack(second_ref, False)

    @pl.when(jnp.logical_not(even_y))
    def _():
        pack(first_ref, False)
        pack(second_ref, True)


def both_sides(strip, j):
    return jnp.where(j == 3, strip, turn(strip, 62))


def beside(v, patch, lane):
    if patch is None:
        return turn(v, 1), turn(v, -1)
    return jnp.where(lane == 0, patch, turn(v, 1)), jnp.where(lane == TX - 1, patch, turn(v, -1))


def patch_of(sides, p):
    return None if p == SRC else turn(sides, -(8 * p + 3))


def given_low(flag, bit, theirs, mine):
    return jnp.where((flag & bit) != 0, jnp.maximum(theirs - mine, 0.0), 0.0)


def given_high(flag, bit, theirs, mine):
    return jnp.where((flag & bit) == 0, jnp.maximum(theirs - mine, 0.0), 0.0)


def coef(flag, bit, low, high, mine):
    return jnp.maximum(mine - jnp.where((flag & bit) != 0, high, low), 0.0)


def coefficients_kernel(
    t_ref, a_ref, f_ref, strip_ref, y0_ref, y1_ref, g_ref, rden_ref, x_ref, edge_ref, row_ref, rows
):
    even_y = is_even("gy")
    blank = jnp.zeros((PAD, TX), F32)
    for k in range(5):
        for p in range(PLANES):
            first, second = y0_ref[k, p], y1_ref[k, p]
            rows[0, k, p, PAD : PAD + Z, :] = jnp.where(even_y, second, first)
            rows[1, k, p, PAD : PAD + Z, :] = jnp.where(even_y, first, second)
            if k < 3:
                for side in range(2):
                    rows[side, k, p, 0:PAD, :] = blank
                    rows[side, k, p, PAD + Z : PAD + Z + PAD, :] = blank

    lane = iota((TY, TX), 1)
    j = lane & 7
    row = iota((TY, TX), 0)

    def refs(p):
        if p < SRC:
            return t_ref.at[p], a_ref.at[p], f_ref.at[p]
        return strip_ref.at[0], strip_ref.at[1], strip_ref.at[2]

    def at_level(z, carry):
        here = level(z)
        below = level(jnp.maximum(z - 1, 0))
        above = level(jnp.minimum(z + 1, Z - 1))
        sides = [both_sides(strip_ref[n, here, :], j) for n in range(3)]

        def halo(side, k, p):
            return jnp.broadcast_to(rows[side, k, p, pl.ds(PAD + z, 1), :], (TY, TX))

        def down(v, h):
            return jnp.where(row == 0, h, pltpu.roll(v, 1, 0))

        def up(v, h):
            return jnp.where(row == TY - 1, h, pltpu.roll(v, TY - 1, 0))

        for p in range(PLANES):
            t_p, a_p, f_p = refs(p)
            t = t_p[here, :]
            f = f_p[here, :].astype(F32)
            a = a_p[here, :]
            tl, tr = beside(t, patch_of(sides[0], p), lane)
            al, ar = beside(a, patch_of(sides[1], p), lane)
            fl, fr = beside(f, patch_of(sides[2], p), lane)
            tu, td = down(t, halo(0, 0, p)), up(t, halo(1, 0, p))
            fu, fd = down(f, halo(0, 1, p)), up(f, halo(1, 1, p))
            au, ad = down(a, halo(0, 2, p)), up(a, halo(1, 2, p))
            tm = jnp.where(z > 0, t_p[below, :], 0.0)
            tp = jnp.where(z < Z - 1, t_p[above, :], 0.0)
            f = f.astype(I32)
            den = 1.0 + coef(f, 1, tl, tr, t) + coef(f, 2, tu, td, t) + coef(f, 4, tm, tp, t)
            rden = 1.0 / den
            shares = [
                given_low(fl.astype(I32), 1, tl, t),
                given_high(fr.astype(I32), 1, tr, t),
                given_low(fu.astype(I32), 2, tu, t),
                given_high(fd.astype(I32), 2, td, t),
                given_low(f_p[below, :].astype(I32), 4, tm, t),
                given_high(f_p[above, :].astype(I32), 4, tp, t),
            ]
            shares = [g * rden for g in shares]
            total = None
            for k, (g, v) in enumerate(zip(shares, (al, ar, au, ad, a_p[below, :], a_p[above, :]))):
                g_ref[k, p, here, :] = g
                total = g * v if total is None else total + g * v
            rden_ref[p, here, :] = rden
            x_ref[p, here, :] = total
        return carry

    lax.fori_loop(0, Z, at_level, 0)

    lane = iota((Z, TX), 1)
    j = lane & 7
    for side in range(2):
        edge = pl.ds(0 if side == 0 else TY - 1, Z, stride=TY)
        sides = [both_sides(rows[side, n, SRC, PAD : PAD + Z, :], j) for n in range(3)]
        for p in range(PLANES):
            t_p, a_p, f_p = refs(p)
            edge_ref[side, p] = g_ref[2 + side, p, edge, :]

            def at(k, shift=0):
                return rows[side, k, p, PAD + shift : PAD + shift + Z, :]

            t, f, a = at(0), at(1), at(2)
            t2, a2 = at(3), at(4)
            t0, f0, a0 = t_p[edge, :], f_p[edge, :].astype(I32), a_p[edge, :]
            tl, tr = beside(t, patch_of(sides[0], p), lane)
            fl, fr = beside(f, patch_of(sides[1], p), lane)
            al, ar = beside(a, patch_of(sides[2], p), lane)
            tm, tp = at(0, -1), at(0, 1)
            f = f.astype(I32)
            low, high = (t2, t0) if side == 0 else (t0, t2)
            den = 1.0 + coef(f, 1, tl, tr, t) + coef(f, 2, low, high, t) + coef(f, 4, tm, tp, t)
            rden = 1.0 / den
            inward = (given_high if side == 0 else given_low)(f0, 2, t0, t)
            total = given_low(fl.astype(I32), 1, tl, t) * al
            total = total + given_high(fr.astype(I32), 1, tr, t) * ar
            total = total + given_low(at(1, -1).astype(I32), 4, tm, t) * at(2, -1)
            total = total + given_high(at(1, 1).astype(I32), 4, tp, t) * at(2, 1)
            total = total + jnp.maximum(t2 - t, 0.0) * a2 + inward * a0
            row_ref[0, side, p] = total * rden
            row_ref[1, side, p] = rden
            row_ref[2, side, p] = inward * rden


def sweeps_kernel(
    rec_ref, g_ref, rden_ref, x_ref, row_ref,
    last_ref, first_ref, second_ref, beyond_ref,
    turned, near, hot, main, wide, levels, adj, adj2, halo,
):
    for c in range(3):
        turned[c] = rec_ref[:, c * TX : (c + 1) * TX].T

    def records(g):
        base = GROUP * (g % 3)
        return [turned[g // 3, base + 8 * k : base + 8 * k + 8, :] for k in range(CAP)], turned[
            g // 3, base + 32 : base + 40, :
        ].astype(I32) - 1

    col8 = iota((TY, TX), 0)
    tall = iota((ROWS, TX), 0)
    across = iota((TX, TX), 0)
    deep = iota((Z, TX), 0)

    def ones(mask):
        return jnp.where(mask, 1.0, 0.0).astype(BF16)

    for dy in (-1, 0, 1):
        for n, dx in enumerate((-1, 0, 1)):
            g = NEAR.index((dx, dy))
            values, cells = records(g)
            for k in range(CAP):
                at = pl.ds((n * CAP + k) * TX, TX)
                cell = cells[k : k + 1, :]
                x = cell & (TX - 1)
                zy = cell >> 7
                if dy == 0:
                    hot[:, at] = ones(tall == zy)
                else:
                    z = jnp.where((zy & 7) == (7 if dy < 0 else 0), cell >> 10, -1)
                    levels[:, at] = ones(deep == z)
                column = (x + 4) & (TX - 1)
                wanted = (col8 == column) & (
                    (col8 < 4) if dx < 0 else (col8 >= 4) if dx > 0 else (col8 >= 0)
                )
                parts = split3(values[k])
                for m in range(3):
                    tiles = []
                    for side in range(2):
                        use = wanted
                        if dx == 0:
                            use = wanted & ((col8 >= 4) if side == 0 else (col8 < 4))
                        for s in range(SRC):
                            if dx == (1 if side == 0 else -1):
                                tiles.append(jnp.zeros((TY, TX), F32))
                            else:
                                tiles.append(jnp.where(use, parts[m][s : s + 1, :], 0.0))
                    near[m, :, at] = jnp.concatenate(tiles, axis=0).astype(BF16)
        onehot = hot[...] if dy == 0 else levels[...]
        strip = dot(onehot, near[0]) + dot(onehot, near[1]) + dot(onehot, near[2])
        if dy == 0:
            last_ref[SRC] = strip * rden_ref[SRC]
        else:
            side = 0 if dy < 0 else 1
            halo[side, SRC] = row_ref[0, side, SRC] + strip * row_ref[1, side, SRC]
            values, cells = records(NEAR.index((0, dy)))
            for k in range(CAP):
                at = pl.ds(k * TX, TX)
                cell = cells[k : k + 1, :]
                zy = cell >> 7
                z = jnp.where((zy & 7) == (7 if dy < 0 else 0), cell >> 10, -1)
                main[0, 0:TX, at] = ones(across == (cell & (TX - 1)))
                parts = split3(values[k])
                mask = deep == z
                for m in range(3):
                    wide[m, :, at] = jnp.concatenate(
                        [jnp.where(mask, parts[m][s : s + 1, :], 0.0) for s in range(SRC)], axis=0
                    ).astype(BF16)
            columns = main[0, 0:TX, :]
            got = dot(wide[0], columns) + dot(wide[1], columns) + dot(wide[2], columns)
            for s in range(SRC):
                halo[side, s] = (
                    row_ref[0, side, s] + got[s * Z : (s + 1) * Z, :] * row_ref[1, side, s]
                )

    values, cells = records(NEAR.index((0, 0)))
    for k in range(CAP):
        at = pl.ds(k * TX, TX)
        cell = cells[k : k + 1, :]
        mask = across == (cell & (TX - 1))
        parts = split3(values[k])
        for m in range(3):
            for s in range(SRC):
                main[m, s * TX : (s + 1) * TX, at] = jnp.where(
                    mask, parts[m][s : s + 1, :], 0.0
                ).astype(BF16)
    onehot = hot[:, CAP * TX : 2 * CAP * TX]
    for s in range(0, SRC, 2):
        two = slice(s * TX, (s + 2) * TX)
        got = dot(onehot, main[0, two, :]) + dot(onehot, main[1, two, :]) + dot(onehot, main[2, two, :])
        last_ref[s] = got[:, :TX] * rden_ref[s]
        last_ref[s + 1] = got[:, TX:] * rden_ref[s + 1]

    for p in range(PLANES):
        adj[p] = x_ref[p] + last_ref[p]
    lane = iota((TY, TX), 1)
    j = lane & 7
    row = iota((TY, TX), 0)

    def sweep(old, new, with_halo):
        def at_level(z, carry):
            here = level(z)
            below = level(jnp.maximum(z - 1, 0))
            above = level(jnp.minimum(z + 1, Z - 1))
            sides = both_sides(old[SRC, here, :], j)
            for p in range(PLANES):
                v = old[p, here, :]
                left, right = beside(v, patch_of(sides, p), lane)
                low, high = 0.0, 0.0
                if with_halo:
                    low = jnp.broadcast_to(halo[0, p, pl.ds(z, 1), :], (TY, TX))
                    high = jnp.broadcast_to(halo[1, p, pl.ds(z, 1), :], (TY, TX))
                down = jnp.where(row == 0, low, pltpu.roll(v, 1, 0))
                up = jnp.where(row == TY - 1, high, pltpu.roll(v, TY - 1, 0))
                total = last_ref[p, here, :]
                for k, w in enumerate((left, right, down, up, old[p, below, :], old[p, above, :])):
                    total = total + g_ref[k, p, here, :] * w
                new[p, here, :] = total
            return carry

        lax.fori_loop(0, Z, at_level, 0)

    sweep(adj, adj2, True)
    sweep(adj2, last_ref, False)

    low, high = pl.ds(0, Z, stride=TY), pl.ds(TY - 1, Z, stride=TY)

    def pack(out, edge):
        total = None
        for p in range(PLANES):
            out[p] = adj2[p, edge, :]
            if p < SRC:
                part = last_ref[p, edge, :]
                total = part if total is None else total + part
        out[PLANES] = total

    even_y = is_even("gy")

    @pl.when(even_y)
    def _():
        pack(first_ref, high)
        pack(second_ref, low)

    @pl.when(jnp.logical_not(even_y))
    def _():
        pack(first_ref, low)
        pack(second_ref, high)

    for side, edge in enumerate((low, high)):
        total = None
        for s in range(SRC):
            part = row_ref[2, side, s] * adj2[s, edge, :]
            total = part if total is None else total + part
        beyond_ref[side] = total


def gradient_kernel(
    last_ref, y0_ref, y1_ref, edge_ref, beyond_ref, slow_ref, adj_ref, grad_ref, fix, above
):
    even_y = is_even("gy")
    for p in range(PLANES + 1):
        first, second = y0_ref[p], y1_ref[p]
        from_low = jnp.where(even_y, second, first)
        from_high = jnp.where(even_y, first, second)
        if p < PLANES:
            fix[0, p] = edge_ref[0, p] * from_low
            fix[1, p] = edge_ref[1, p] * from_high
        else:
            above[0] = beyond_ref[0] + from_low
            above[1] = beyond_ref[1] + from_high
    lane = iota((TY, TX), 1)
    row = iota((TY, TX), 0)

    def at_level(z, carry):
        here = level(z)

        def wide(ref, *index):
            return jnp.broadcast_to(ref[(*index, pl.ds(z, 1), slice(None))], (TY, TX))

        total = None
        for p in range(PLANES):
            v = last_ref[p, here, :]
            v = v + jnp.where(row == 0, wide(fix, 0, p), jnp.where(row == TY - 1, wide(fix, 1, p), 0.0))
            if p < SRC:
                adj_ref[p, here, :] = v
                total = v if total is None else total + v
            else:
                strip = v
        for by in (8, 16, 32):
            strip = strip + turn(strip, by)
        left = jnp.where(lane == 0, turn(strip, -59), turn(total, 1))
        right = jnp.where(lane == TX - 1, turn(strip, 3), turn(total, -1))
        down = jnp.where(row == 0, wide(above, 0), pltpu.roll(total, 1, 0))
        up = jnp.where(row == TY - 1, wide(above, 1), pltpu.roll(total, TY - 1, 0))
        beside_it = right + left + up + down
        grad_ref[here, :] = slow_ref[here, :] * (total + 0.125 * (beside_it - 4.0 * total))
        return carry

    lax.fori_loop(0, Z, at_level, 0)


def call(kernel, outs, scratch, flops, name):
    vmem = pl.BlockSpec(memory_space=pltpu.VMEM)

    def run(*args):
        moved = sum(a.size * 4 for a in args)
        return pl.pallas_call(
            kernel,
            name=name,
            out_shape=[jax.ShapeDtypeStruct(s, F32) for s in outs],
            in_specs=[vmem] * len(args),
            out_specs=[vmem] * len(outs),
            scratch_shapes=scratch,
            compiler_params=pltpu.CompilerParams(vmem_limit_bytes=24 << 20),
            cost_estimate=pl.CostEstimate(flops=flops, bytes_accessed=moved, transcendentals=0),
        )(*args)

    return run


def swapped(v, axis, count, odd):
    pairs = [(i, i + 1) for i in range(odd, count - 1, 2)]
    return lax.ppermute(v, axis, [(a, b) for a, b in pairs] + [(b, a) for a, b in pairs])


def shards(traveltime, adjoint_start, upwind_flags, slowness, residual_rows, station_tile, station_cell):
    devices = lax.axis_size(("gx", "gy"))
    nx, ny = lax.axis_size("gx"), lax.axis_size("gy")
    count = residual_rows.shape[0]
    t, a, f = (v.reshape(SRC, ROWS, TX) for v in (traveltime, adjoint_start, upwind_flags))

    (sent,) = call(
        records_kernel,
        [(devices, 3 * TX)],
        [pltpu.VMEM((3, GROUP, count), F32), pltpu.VMEM((devices + 64, TX), F32)],
        10**6,
        "records",
    )(residual_rows.T, station_tile.reshape(1, count), station_cell.reshape(1, count))

    x_out0, x_out1, own = call(
        edges_kernel, [(ROWS, TX), (ROWS, TX), (3, ROWS, TX)], [], 10**6, "edges"
    )(t, a, f)
    x_in0 = swapped(x_out0, "gx", nx, 0)
    x_in1 = swapped(x_out1, "gx", nx, 1)

    strip, y_out0, y_out1 = call(
        strips_kernel,
        [(3, ROWS, TX), (5, PLANES, Z, TX), (5, PLANES, Z, TX)],
        [],
        10**6,
        "strips",
    )(t, a, f, own, x_in0, x_in1)
    y_in0 = swapped(y_out0, "gy", ny, 0)
    y_in1 = swapped(y_out1, "gy", ny, 1)

    got = lax.all_to_all(sent, ("gx", "gy"), 0, 0, tiled=True)

    g, rden, x1, edge, halo_rows = call(
        coefficients_kernel,
        [
            (6, PLANES, ROWS, TX),
            (PLANES, ROWS, TX),
            (PLANES, ROWS, TX),
            (2, PLANES, Z, TX),
            (3, 2, PLANES, Z, TX),
        ],
        [pltpu.VMEM((2, 5, PLANES, Z + 2 * PAD, TX), F32)],
        10**7,
        "coefficients",
    )(t, a, f, strip, y_in0, y_in1)

    depth = CAP * TX
    last, e_out0, e_out1, beyond = call(
        sweeps_kernel,
        [
            (PLANES, ROWS, TX),
            (PLANES + 1, Z, TX),
            (PLANES + 1, Z, TX),
            (2, Z, TX),
        ],
        [
            pltpu.VMEM((3, TX, TX), F32),
            pltpu.VMEM((3, TX, 3 * depth), BF16),
            pltpu.VMEM((ROWS, 3 * depth), BF16),
            pltpu.VMEM((3, SRC * TX, depth), BF16),
            pltpu.VMEM((3, SRC * Z, depth), BF16),
            pltpu.VMEM((Z, 3 * depth), BF16),
            pltpu.VMEM((PLANES, ROWS, TX), F32),
            pltpu.VMEM((PLANES, ROWS, TX), F32),
            pltpu.VMEM((2, PLANES, Z, TX), F32),
        ],
        10**7,
        "sweeps",
    )(got, g, rden, x1, halo_rows)
    e_in0 = swapped(e_out0, "gy", ny, 0)
    e_in1 = swapped(e_out1, "gy", ny, 1)

    adjoint, gradient = call(
        gradient_kernel,
        [(SRC, ROWS, TX), (ROWS, TX)],
        [pltpu.VMEM((2, PLANES, Z, TX), F32), pltpu.VMEM((2, Z, TX), F32)],
        10**6,
        "gradient",
    )(last, e_in0, e_in1, edge, beyond, slowness.reshape(ROWS, TX))
    return adjoint.reshape(traveltime.shape), gradient.reshape(slowness.shape)


def solution(mesh):
    placed = (
        P(None, None, "gy", "gx"),
        P(None, None, "gy", "gx"),
        P(None, None, "gy", "gx"),
        P(None, "gy", "gx"),
        P(("gx", "gy"), None),
        P(("gx", "gy"), None),
        P(("gx", "gy")),
    )
    return jax.shard_map(
        shards,
        mesh=mesh,
        in_specs=placed,
        out_specs=(P(None, None, "gy", "gx"), P(None, "gy", "gx")),
        check_vma=False,
    )
```

```python
import jax
import jax.numpy as jnp
from jax import lax
from jax.experimental import pallas as pl
from jax.experimental.pallas import tpu as pltpu
from jax.sharding import PartitionSpec as P


F32 = jnp.float32
BF16 = jnp.bfloat16
I32 = jnp.int32

SRC = 8
Z = 32
TY = 8
TX = 128
PLANES = SRC + 1
ROWS = Z * TY
HALO = 4
CAP = 4
SPLIT = 2
GROUP = 40
PART = 64
LEAVING_LIMIT = 52
RECORDS_LIMIT = 56
CORE_LIMIT = 51
PAD = 8
NEAR = tuple((dx, dy) for dx in (-1, 0, 1) for dy in (-1, 0, 1))

NT = (((1,), (1,)), ((), ()))
NN = (((1,), (0,)), ((), ()))


def iota(shape, dim):
    return lax.broadcasted_iota(I32, shape, dim)


def turn(v, by):
    return pltpu.roll(v, by % TX, 1)


def level(z):
    return pl.ds(pl.multiple_of(z * TY, TY), TY)


def cat(parts):
    return jnp.concatenate(parts, axis=0)


def dot(a, b, dims=NT):
    return lax.dot_general(a, b, dims, preferred_element_type=F32)


def split(v, count):
    parts = []
    for _ in range(count - 1):
        parts.append(v.astype(BF16).astype(F32))
        v = v - parts[-1]
    return [*parts, v]


def all_start(copies):
    for copy in copies:
        copy.start()


def all_wait(copies):
    for copy in copies:
        copy.wait()


def is_even(axis):
    return lax.rem(lax.axis_index(axis), 2) == 0


def records_kernel(
    rows_hbm, tile_hbm, cell_hbm, out_ref, rows_ref, tile_ref, cell_ref, parts, shifted, sems
):
    pairs = ((tile_hbm, tile_ref), (rows_hbm, rows_ref), (cell_hbm, cell_ref))
    coming = [pltpu.make_async_copy(hbm, ref, sems.at[n]) for n, (hbm, ref) in enumerate(pairs)]
    all_start(coming)
    shifted[...] = jnp.zeros(shifted.shape, F32)
    count = rows_ref.shape[1]
    devices = out_ref.shape[0] // 3
    all_wait(coming)
    named = (iota((devices, count), 0) == tile_ref[...]).astype(F32)
    earlier = (iota((count, count), 0) < iota((count, count), 1)).astype(F32).astype(BF16)
    picks = named.astype(BF16)
    before = dot(picks, earlier, NN)
    rank = jnp.sum(before * named, axis=0, keepdims=True).astype(I32)
    values = rows_ref[...]
    cells = (cell_ref[...] + 1).astype(F32)
    blocks = [jnp.where(rank == k, values, 0.0) for k in range(CAP)]
    blocks.append(jnp.where(rank == iota((8, count), 0), cells, 0.0))
    for k, block in enumerate(blocks):
        for n, part in enumerate(split(block, 3)):
            parts[n, 8 * k : 8 * k + 8, :] = part
    own = sum(dot(picks, parts[n].astype(BF16)) for n in range(3))
    shifted[32 : 32 + devices, 0:GROUP] = own
    lane = iota((devices, TX), 1)
    ty = lax.rem(iota((devices, TX), 0), 16)
    for c in range(3):
        chunk = jnp.zeros((devices, TX), F32)
        for i in range(3):
            dx, dy = NEAR[3 * c + i]
            off = 32 + 16 * dx + dy
            theirs = shifted[off : off + devices, :]
            held = (lane >= GROUP * i) & (lane < GROUP * (i + 1))
            if dy:
                held = held & (ty + dy >= 0) & (ty + dy < 16)
            chunk = jnp.where(held, turn(theirs, GROUP * i) if i else theirs, chunk)
        out_ref[pl.ds(c, devices, stride=3), :] = chunk


def edge_rows(out, t, a, f, high):
    edge = pl.ds(TY - 1 if high else 0, Z, stride=TY)
    inner = pl.ds(TY - 2 if high else 1, Z, stride=TY)
    out[0][...] = t[edge, :]
    out[1][...] = f[edge, :].astype(F32)
    out[2][...] = a[edge, :]
    out[3][...] = t[inner, :]
    up = (f[inner, :] & 2) != 0
    given = a[inner, :]
    out[4][...] = jnp.where(up, given, 0.0) if high else jnp.where(up, 0.0, given)


def by_parity(axis, first, second, fill):
    even = is_even(axis)

    @pl.when(even)
    def _():
        fill(first, True)
        fill(second, False)

    @pl.when(jnp.logical_not(even))
    def _():
        fill(first, False)
        fill(second, True)


def leaving_kernel(
    t_hbm, a_hbm, f_hbm,
    x0_ref, x1_ref, y0_ref, y1_ref, own_ref,
    t_ref, a_ref, f_ref, sems,
):
    arrays = ((t_hbm, t_ref), (a_hbm, a_ref), (f_hbm, f_ref))

    def copies(c):
        part = pl.ds(c * PART, PART)
        return [
            pltpu.make_async_copy(hbm.at[:, part, :], ref.at[:, part, :], sems.at[n, c])
            for n, (hbm, ref) in enumerate(arrays)
        ]

    for c in range(ROWS // PART):
        for copy in copies(c):
            copy.start()

    even = is_even("gx")
    lane = iota((TY, TX), 1)
    j = lane & 7

    def at_level(z, carry):
        here = level(z)
        packed = []
        for n, ref in enumerate((t_ref, a_ref, f_ref)):
            both = None
            for s in range(SRC):
                v = turn(ref[s, here, :].astype(F32), HALO + 8 * s)
                both = v if both is None else jnp.where(lane >> 3 == s, v, both)
            own_ref[n, here, :] = both
            packed.append(both)
        t, a, f = packed
        f = turn(f, 64)
        to_right = jnp.where(lane < 64, jnp.where(j < 4, t, turn(a, 4)), f)
        to_left = jnp.where(lane < 64, jnp.where(j < 4, turn(t, -4), a), f)
        x0_ref[here, :] = jnp.where(even, to_right, to_left)
        x1_ref[here, :] = jnp.where(even, to_left, to_right)
        return carry

    for c in range(ROWS // PART):
        for copy in copies(c):
            copy.wait()
        levels = PART // TY
        lax.fori_loop(c * levels, (c + 1) * levels, at_level, 0, unroll=8)

    def rows(out, high):
        for p in range(SRC):
            edge_rows([out.at[k, p] for k in range(5)], t_ref.at[p], a_ref.at[p], f_ref.at[p], high)

    by_parity("gy", y0_ref, y1_ref, rows)


def strips_kernel(
    own_ref, x0_ref, x1_ref, strip_out, y0_ref, y1_ref, strip_ref, f_ref, sems
):
    even = is_even("gx")
    shape = (ROWS, TX)
    lane = iota(shape, 1)
    near = (lane & 7) < 4
    low = lane < 64
    x0, x1 = x0_ref[...], x1_ref[...]
    left = jnp.where(even, x1, x0)
    right = jnp.where(even, x0, x1)
    t, a, f = own_ref[0], own_ref[1], own_ref[2]
    strip_ref[0] = jnp.where(
        low, jnp.where(near, left, t), turn(jnp.where(near, t, turn(right, 4)), 64)
    )
    strip_ref[1] = jnp.where(
        low, jnp.where(near, turn(left, -4), a), turn(jnp.where(near, a, right), 64)
    )
    flags = jnp.where(low, jnp.where(near, turn(left, 64), f), jnp.where(near, turn(f, 64), right))
    strip_ref[2] = flags
    f_ref[...] = flags.astype(I32)
    going = pltpu.make_async_copy(strip_ref, strip_out, sems.at[0])
    going.start()

    def rows(out, high):
        edge_rows([out.at[k] for k in range(5)], strip_ref.at[0], strip_ref.at[1], f_ref, high)

    by_parity("gy", y0_ref, y1_ref, rows)
    going.wait()


def both_sides(strip):
    return jnp.where((iota(strip.shape, 1) & 7) == 3, strip, turn(strip, 62))


def beside(v, patch, lane):
    if patch is None:
        return turn(v, 1), turn(v, -1)
    return jnp.where(lane == 0, patch, turn(v, 1)), jnp.where(lane == TX - 1, patch, turn(v, -1))


def patch_of(sides, p):
    return None if p == SRC else turn(sides, -(8 * p + 3))


def given_low(flag, bit, theirs, mine):
    return jnp.where((flag & bit) != 0, jnp.maximum(theirs - mine, 0.0), 0.0)


def given_high(flag, bit, theirs, mine):
    return jnp.where((flag & bit) == 0, jnp.maximum(theirs - mine, 0.0), 0.0)


def coef(flag, bit, low, high, mine):
    return jnp.maximum(mine - jnp.where((flag & bit) != 0, high, low), 0.0)


def take_rows(first, second, rows, flags, p, k):
    even = is_even("gy")
    here = pl.ds(PAD, Z)
    for side in range(2):
        v = jnp.where(even, second, first) if side == 0 else jnp.where(even, first, second)
        if k == 1:
            flags[side, p, here, :] = v.astype(I32)
        else:
            rows[side, k, p, here, :] = v


def shares_at(z, p, refs, sides, rows, flags, lane, row):
    t_p, a_p, f_p = refs
    here = level(z)
    below = level(jnp.maximum(z - 1, 0))
    above = level(jnp.minimum(z + 1, Z - 1))

    def halo(ref, *index):
        return jnp.broadcast_to(ref[(*index, pl.ds(PAD + z, 1), slice(None))], (TY, TX))

    def down(v, h):
        return jnp.where(row == 0, h, pltpu.roll(v, 1, 0))

    def up(v, h):
        return jnp.where(row == TY - 1, h, pltpu.roll(v, TY - 1, 0))

    t, f, a = t_p[here, :], f_p[here, :], a_p[here, :]
    tl, tr = beside(t, sides[0], lane)
    al, ar = beside(a, sides[1], lane)
    fl, fr = beside(f, sides[2], lane)
    tu, td = down(t, halo(rows, 0, 0, p)), up(t, halo(rows, 1, 0, p))
    fu, fd = down(f, halo(flags, 0, p)), up(f, halo(flags, 1, p))
    au, ad = down(a, halo(rows, 0, 2, p)), up(a, halo(rows, 1, 2, p))
    tm = jnp.where(z > 0, t_p[below, :], 0.0)
    tp = jnp.where(z < Z - 1, t_p[above, :], 0.0)
    den = 1.0 + coef(f, 1, tl, tr, t) + coef(f, 2, tu, td, t) + coef(f, 4, tm, tp, t)
    rden = 1.0 / den
    shares = [
        given_low(fl, 1, tl, t),
        given_high(fr, 1, tr, t),
        given_low(fu, 2, tu, t),
        given_high(fd, 2, td, t),
        given_low(f_p[below, :], 4, tm, t),
        given_high(f_p[above, :], 4, tp, t),
    ]
    shares = [g * rden for g in shares]
    total = None
    for g, v in zip(shares, (al, ar, au, ad, a_p[below, :], a_p[above, :])):
        total = g * v if total is None else total + g * v
    return shares, rden, total


def ones(mask):
    return jnp.where(mask, 1.0, 0.0).astype(BF16)


def scatter(rec_ref, main_ref, strip_ref, row_ref, turned, hot, levels, near, wide, spots):
    for c in range(3):
        turned[c] = rec_ref[pl.ds(c, TX, stride=3), :].T

    def held(dx, dy):
        g = NEAR.index((dx, dy))
        base = GROUP * (g % 3)
        values = [turned[g // 3, base + 8 * k : base + 8 * k + 8, :] for k in range(CAP)]
        return values, turned[g // 3, base + 32 : base + 40, :].astype(I32) - 1

    j = iota((TY, TX), 0)
    tall = iota((ROWS, TX), 0)
    deep = iota((Z, TX), 0)
    spread = iota((TY * TX, TX), 0)
    depth = CAP * TX
    for dy in (0, -1, 1):
        for n, dx in enumerate((-1, 0, 1)):
            values, cells = held(dx, dy)
            for k in range(CAP):
                cell = cells[k : k + 1, :]
                x = cell & (TX - 1)
                y = (cell >> 7) & (TY - 1)
                z = cell >> 10
                at = pl.ds(n * depth + k * TX, TX)
                if dy == 0:
                    hot[:, at] = ones(tall == cell >> 7)
                else:
                    z = jnp.where(y == (TY - 1 if dy < 0 else 0), z, -1)
                    levels[:, at] = ones(deep == z)
                parts = split(values[k], SPLIT)
                column = j == ((x + HALO) & (TX - 1))
                for side in range(2):
                    if dx == (1 if side == 0 else -1):
                        continue
                    inner = (dx == 0) == (side == 0)
                    use = column & ((j >= HALO) if inner else (j < HALO))
                    to = pl.ds((n - side) * depth + k * TX, TX)
                    for m in range(SPLIT):
                        for s in range(0, SRC, 2):
                            two = [jnp.where(use, parts[m][i : i + 1, :], 0.0) for i in (s, s + 1)]
                            near[side, m, 8 * s : 8 * s + 16, to] = cat(two).astype(BF16)
                if dx == 0:
                    to = pl.ds(k * TX, TX)
                    mask = deep == z
                    for m in range(SPLIT):
                        for s in range(SRC):
                            one = jnp.where(mask, parts[m][s : s + 1, :], 0.0)
                            wide[m, s * Z : (s + 1) * Z, to] = one.astype(BF16)
                    if dy == 0:
                        spots[:, to] = ones(spread == (cell & (TY * TX - 1)))
                    else:
                        spots[0:TX, to] = ones(iota((TX, TX), 0) == x)
        onehot = hot[...] if dy == 0 else levels[...]
        halves = []
        for side in range(2):
            some = onehot[:, side * depth : (side + 2) * depth]
            halves.append(sum(dot(some, near[side, m]) for m in range(SPLIT)))
        strip = jnp.concatenate(halves, axis=1)
        if dy == 0:
            strip_ref[...] = strip
            for y in range(0, TY, 2):
                some = spots[y * TX : (y + 2) * TX, :]
                got = sum(dot(wide[m], some) for m in range(SPLIT))
                for i in range(2):
                    for s in range(SRC):
                        main_ref[s, pl.ds(y + i, Z, stride=TY), :] = got[
                            s * Z : (s + 1) * Z, i * TX : (i + 1) * TX
                        ]
        else:
            side = 0 if dy < 0 else 1
            row_ref[side, SRC] = strip
            got = sum(dot(wide[m], spots[0:TX, :]) for m in range(SPLIT))
            for s in range(SRC):
                row_ref[side, s] = got[s * Z : (s + 1) * Z, :]


def core_kernel(
    rec_hbm, t_hbm, a_hbm, f_hbm, strip_hbm, y0_hbm, y1_hbm, h0_hbm, h1_hbm,
    last_ref, e0_ref, e1_ref, edge_ref, beyond_ref,
    rec_ref, t_ref, a_ref, f_ref, strip_in, y0_ref, y1_ref, h0_ref, h1_ref, strip_flags,
    turned, hot, levels, near, wide, spots, rows, flags, both, both_flags,
    g_ref, halo, back, adj, adj2, sems,
):
    pairs = (
        (rec_hbm, rec_ref),
        (y0_hbm, y0_ref),
        (y1_hbm, y1_ref),
        (strip_hbm, strip_in),
        (h0_hbm, h0_ref),
        (h1_hbm, h1_ref),
        (t_hbm, t_ref),
        (f_hbm, f_ref),
        (a_hbm, a_ref),
    )
    coming = [pltpu.make_async_copy(hbm, ref, sems.at[n]) for n, (hbm, ref) in enumerate(pairs)]
    all_start(coming)
    coming[0].wait()
    scatter(rec_ref, last_ref, last_ref.at[SRC], halo, turned, hot, levels, near, wide, spots)
    all_wait(coming[1:6])

    blank = jnp.zeros((PAD, TX), F32)
    for p in range(PLANES):
        for k in range(5):
            if p == SRC:
                take_rows(h0_ref[k], h1_ref[k], rows, flags, p, k)
            else:
                take_rows(y0_ref[k, p], y1_ref[k, p], rows, flags, p, k)
        for side in range(2):
            for k in (0, 2):
                rows[side, k, p, 0:PAD, :] = blank
                rows[side, k, p, PAD + Z : PAD + Z + PAD, :] = blank
    strip_flags[...] = strip_in[2].astype(I32)
    both[0] = both_sides(strip_in[0])
    both[1] = both_sides(strip_in[1])
    both_flags[...] = both_sides(strip_flags[...])
    lane = iota((TY, TX), 1)
    row = iota((TY, TX), 0)
    all_wait(coming[6:])

    def refs(p):
        if p < SRC:
            return t_ref.at[p], a_ref.at[p], f_ref.at[p]
        return strip_in.at[0], strip_in.at[1], strip_flags

    def at_level(z, carry):
        here = level(z)
        pair = [both[0, here, :], both[1, here, :], both_flags[here, :]]
        for p in range(PLANES):
            sides = [patch_of(v, p) for v in pair]
            shares, rden, total = shares_at(z, p, refs(p), sides, rows, flags, lane, row)
            for k, g in enumerate(shares):
                g_ref[k, p, here, :] = g
            source = last_ref[p, here, :] * rden
            last_ref[p, here, :] = source
            adj[p, here, :] = total + source
        return carry

    lax.fori_loop(0, Z, at_level, 0, unroll=2)

    wide_lane = iota((Z, TX), 1)
    for side in range(2):
        edge = pl.ds(0 if side == 0 else TY - 1, Z, stride=TY)
        here = pl.ds(PAD, Z)
        pair = [
            both_sides(rows[side, 0, SRC, here, :]),
            both_sides(rows[side, 2, SRC, here, :]),
            both_sides(flags[side, SRC, here, :]),
        ]
        for p in range(PLANES):
            t_p, a_p, f_p = refs(p)
            edge_ref[side, p] = g_ref[2 + side, p, edge, :]

            def at(k, shift=0):
                return rows[side, k, p, PAD + shift : PAD + shift + Z, :]

            t, a, f = at(0), at(2), flags[side, p, here, :]
            t2, a2 = at(3), at(4)
            t0, f0, a0 = t_p[edge, :], f_p[edge, :], a_p[edge, :]
            tl, tr = beside(t, patch_of(pair[0], p), wide_lane)
            al, ar = beside(a, patch_of(pair[1], p), wide_lane)
            fl, fr = beside(f, patch_of(pair[2], p), wide_lane)
            tm, tp = at(0, -1), at(0, 1)
            fm = flags[side, p, PAD - 1 : PAD - 1 + Z, :]
            fp = flags[side, p, PAD + 1 : PAD + 1 + Z, :]
            low, high = (t2, t0) if side == 0 else (t0, t2)
            den = 1.0 + coef(f, 1, tl, tr, t) + coef(f, 2, low, high, t) + coef(f, 4, tm, tp, t)
            rden = 1.0 / den
            inward = (given_high if side == 0 else given_low)(f0, 2, t0, t)
            total = halo[side, p] + given_low(fl, 1, tl, t) * al
            total = total + given_high(fr, 1, tr, t) * ar
            total = total + given_low(fm, 4, tm, t) * at(2, -1)
            total = total + given_high(fp, 4, tp, t) * at(2, 1)
            total = total + jnp.maximum(t2 - t, 0.0) * a2 + inward * a0
            halo[side, p] = total * rden
            back[side, p] = inward * rden

    def sweep(old, new, with_halo):
        both[0] = both_sides(old[SRC])

        def at_level(z, carry):
            here = level(z)
            below = level(jnp.maximum(z - 1, 0))
            above = level(jnp.minimum(z + 1, Z - 1))
            sides = both[0, here, :]
            for p in range(PLANES):
                v = old[p, here, :]
                left, right = beside(v, patch_of(sides, p), lane)
                low, high = 0.0, 0.0
                if with_halo:
                    low = jnp.broadcast_to(halo[0, p, pl.ds(z, 1), :], (TY, TX))
                    high = jnp.broadcast_to(halo[1, p, pl.ds(z, 1), :], (TY, TX))
                down = jnp.where(row == 0, low, pltpu.roll(v, 1, 0))
                up = jnp.where(row == TY - 1, high, pltpu.roll(v, TY - 1, 0))
                total = last_ref[p, here, :]
                for k, w in enumerate((left, right, down, up, old[p, below, :], old[p, above, :])):
                    total = total + g_ref[k, p, here, :] * w
                new[p, here, :] = total
            return carry

        lax.fori_loop(0, Z, at_level, 0, unroll=4)

    sweep(adj, adj2, True)
    sweep(adj2, last_ref, False)

    low, high = pl.ds(0, Z, stride=TY), pl.ds(TY - 1, Z, stride=TY)

    def pack(out, up):
        edge = high if up else low
        total = None
        for p in range(PLANES):
            out[p] = adj2[p, edge, :]
            if p < SRC:
                part = last_ref[p, edge, :]
                total = part if total is None else total + part
        out[PLANES] = total

    by_parity("gy", e0_ref, e1_ref, pack)
    for side, edge in enumerate((low, high)):
        total = None
        for s in range(SRC):
            part = back[side, s] * adj2[s, edge, :]
            total = part if total is None else total + part
        beyond_ref[side] = total


def gradient_kernel(
    last_ref, y0_ref, y1_ref, edge_ref, beyond_ref, slow_ref, adj_ref, grad_ref, fix, above, patch
):
    even_y = is_even("gy")
    for p in range(PLANES + 1):
        first, second = y0_ref[p], y1_ref[p]
        from_low = jnp.where(even_y, second, first)
        from_high = jnp.where(even_y, first, second)
        if p < PLANES:
            fix[0, p] = edge_ref[0, p] * from_low
            fix[1, p] = edge_ref[1, p] * from_high
        else:
            above[0] = beyond_ref[0] + from_low
            above[1] = beyond_ref[1] + from_high
    lane = iota((TY, TX), 1)
    row = iota((TY, TX), 0)

    def wide(ref, z, *index):
        return jnp.broadcast_to(ref[(*index, pl.ds(z, 1), slice(None))], (TY, TX))

    def completed(z, p):
        low, high = wide(fix, z, 0, p), wide(fix, z, 1, p)
        return last_ref[p, level(z), :] + jnp.where(
            row == 0, low, jnp.where(row == TY - 1, high, 0.0)
        )

    def strip_level(z, carry):
        patch[level(z), :] = completed(z, SRC)
        return carry

    lax.fori_loop(0, Z, strip_level, 0, unroll=8)
    strip = patch[...]
    for by in (8, 16, 32):
        strip = strip + turn(strip, by)
    patch[...] = jnp.where(iota((ROWS, TX), 1) == 0, turn(strip, -59), turn(strip, 3))

    def at_level(z, carry):
        here = level(z)
        total = None
        for p in range(SRC):
            v = completed(z, p)
            adj_ref[p, here, :] = v
            total = v if total is None else total + v
        left, right = beside(total, patch[here, :], lane)
        down = jnp.where(row == 0, wide(above, z, 0), pltpu.roll(total, 1, 0))
        up = jnp.where(row == TY - 1, wide(above, z, 1), pltpu.roll(total, TY - 1, 0))
        beside_it = right + left + up + down
        grad_ref[here, :] = slow_ref[here, :] * (total + 0.125 * (beside_it - 4.0 * total))
        return carry

    lax.fori_loop(0, Z, at_level, 0, unroll=4)


def f32(*shape):
    return jax.ShapeDtypeStruct(shape, F32)


def call(kernel, outs, scratch, flops, ins=(), outs_in=(), limit=20):
    vmem = pl.BlockSpec(memory_space=pltpu.VMEM)

    def run(*args):
        moved = sum(a.size * 4 for a in args)
        given = [pl.BlockSpec(memory_space=s) for s in ins]
        kept = [pl.BlockSpec(memory_space=s) for s in outs_in]
        return pl.pallas_call(
            kernel,
            out_shape=outs,
            in_specs=given + [vmem] * (len(args) - len(given)),
            out_specs=kept + [vmem] * (len(outs) - len(kept)),
            scratch_shapes=scratch,
            compiler_params=pltpu.CompilerParams(vmem_limit_bytes=limit << 20),
            cost_estimate=pl.CostEstimate(flops=flops, bytes_accessed=moved, transcendentals=0),
        )(*args)

    return run


def swapped(v, axis, count, odd):
    pairs = [(i, i + 1) for i in range(odd, count - 1, 2)]
    return lax.ppermute(v, axis, [(a, b) for a, b in pairs] + [(b, a) for a, b in pairs])


def shards(traveltime, adjoint_start, upwind_flags, slowness, residual_rows, station_tile, station_cell):
    devices = lax.axis_size(("gx", "gy"))
    nx, ny = lax.axis_size("gx"), lax.axis_size("gy")
    count = residual_rows.shape[0]
    t, a, f = (v.reshape(SRC, ROWS, TX) for v in (traveltime, adjoint_start, upwind_flags))
    whole = (SRC, ROWS, TX)

    x_out0, x_out1, y_out0, y_out1, own = call(
        leaving_kernel,
        [
            f32(ROWS, TX),
            f32(ROWS, TX),
            f32(5, SRC, Z, TX),
            f32(5, SRC, Z, TX),
            f32(3, ROWS, TX),
        ],
        [
            pltpu.VMEM(whole, F32),
            pltpu.VMEM(whole, F32),
            pltpu.VMEM(whole, I32),
            pltpu.SemaphoreType.DMA((3, ROWS // PART)),
        ],
        10**6,
        ins=[pltpu.HBM] * 3,
        limit=LEAVING_LIMIT,
    )(t, a, f)
    x_in0 = swapped(x_out0, "gx", nx, 0)
    x_in1 = swapped(x_out1, "gx", nx, 1)
    y_in0 = swapped(y_out0, "gy", ny, 0)
    y_in1 = swapped(y_out1, "gy", ny, 1)
    (sent,) = call(
        records_kernel,
        [f32(devices * 3, TX)],
        [
            pltpu.VMEM((SRC, count), F32),
            pltpu.VMEM((1, count), I32),
            pltpu.VMEM((1, count), I32),
            pltpu.VMEM((3, GROUP, count), F32),
            pltpu.VMEM((devices + 64, TX), F32),
            pltpu.SemaphoreType.DMA((3,)),
        ],
        10**6,
        ins=[pltpu.HBM] * 3,
        limit=RECORDS_LIMIT,
    )(residual_rows.T, station_tile.reshape(1, count), station_cell.reshape(1, count))
    got = lax.all_to_all(sent.reshape(devices, 1, 3 * TX), ("gx", "gy"), 0, 0, tiled=True)
    got = got.reshape(devices * 3, TX)

    strip, h_out0, h_out1 = call(
        strips_kernel,
        [f32(3, ROWS, TX), f32(5, Z, TX), f32(5, Z, TX)],
        [
            pltpu.VMEM((3, ROWS, TX), F32),
            pltpu.VMEM((ROWS, TX), I32),
            pltpu.SemaphoreType.DMA((1,)),
        ],
        10**6,
        outs_in=[pltpu.HBM],
    )(own, x_in0, x_in1)
    h_in0 = swapped(h_out0, "gy", ny, 0)
    h_in1 = swapped(h_out1, "gy", ny, 1)

    depth = CAP * TX
    last, e_out0, e_out1, edges, beyond = call(
        core_kernel,
        [
            f32(PLANES, ROWS, TX),
            f32(PLANES + 1, Z, TX),
            f32(PLANES + 1, Z, TX),
            f32(2, PLANES, Z, TX),
            f32(2, Z, TX),
        ],
        [
            pltpu.VMEM((devices * 3, TX), F32),
            pltpu.VMEM(whole, F32),
            pltpu.VMEM(whole, F32),
            pltpu.VMEM(whole, I32),
            pltpu.VMEM((3, ROWS, TX), F32),
            pltpu.VMEM((5, SRC, Z, TX), F32),
            pltpu.VMEM((5, SRC, Z, TX), F32),
            pltpu.VMEM((5, Z, TX), F32),
            pltpu.VMEM((5, Z, TX), F32),
            pltpu.VMEM((ROWS, TX), I32),
            pltpu.VMEM((3, TX, TX), F32),
            pltpu.VMEM((ROWS, 3 * depth), BF16),
            pltpu.VMEM((Z, 3 * depth), BF16),
            pltpu.VMEM((2, SPLIT, SRC * 8, 2 * depth), BF16),
            pltpu.VMEM((SPLIT, SRC * Z, depth), BF16),
            pltpu.VMEM((TY * TX, depth), BF16),
            pltpu.VMEM((2, 5, PLANES, Z + 2 * PAD, TX), F32),
            pltpu.VMEM((2, PLANES, Z + 2 * PAD, TX), I32),
            pltpu.VMEM((2, ROWS, TX), F32),
            pltpu.VMEM((ROWS, TX), I32),
            pltpu.VMEM((6, PLANES, ROWS, TX), F32),
            pltpu.VMEM((2, PLANES, Z, TX), F32),
            pltpu.VMEM((2, PLANES, Z, TX), F32),
            pltpu.VMEM((PLANES, ROWS, TX), F32),
            pltpu.VMEM((PLANES, ROWS, TX), F32),
            pltpu.SemaphoreType.DMA((9,)),
        ],
        10**8,
        ins=[pltpu.HBM] * 9,
        limit=CORE_LIMIT,
    )(got, t, a, f, strip, y_in0, y_in1, h_in0, h_in1)
    e_in0 = swapped(e_out0, "gy", ny, 0)
    e_in1 = swapped(e_out1, "gy", ny, 1)

    adjoint, gradient = call(
        gradient_kernel,
        [f32(*whole), f32(ROWS, TX)],
        [
            pltpu.VMEM((2, PLANES, Z, TX), F32),
            pltpu.VMEM((2, Z, TX), F32),
            pltpu.VMEM((ROWS, TX), F32),
        ],
        10**6,
    )(last, e_in0, e_in1, edges, beyond, slowness.reshape(ROWS, TX))
    return adjoint.reshape(traveltime.shape), gradient.reshape(slowness.shape)


def solution(mesh):
    placed = (
        P(None, None, "gy", "gx"),
        P(None, None, "gy", "gx"),
        P(None, None, "gy", "gx"),
        P(None, "gy", "gx"),
        P(("gx", "gy"), None),
        P(("gx", "gy"), None),
        P(("gx", "gy")),
    )

    return jax.shard_map(
        shards,
        mesh=mesh,
        in_specs=placed,
        out_specs=(P(None, None, "gy", "gx"), P(None, "gy", "gx")),
        check_vma=False,
    )
```

```python
import jax
import jax.numpy as jnp
from jax import lax
from jax.experimental import pallas as pl
from jax.experimental.pallas import tpu as pltpu
from jax.sharding import PartitionSpec as P


F32 = jnp.float32
BF16 = jnp.bfloat16
I32 = jnp.int32

SRC = 8
Z = 32
TY = 8
TX = 128
PLANES = SRC + 1
ROWS = Z * TY
HALO = 4
CAP = 4
SPLIT = 2
GROUP = 40
PART = 64
LEAVING_LIMIT = 52
RECORDS_LIMIT = 56
CORE_LIMIT = 51
GRADIENT_LIMIT = 52.5
PAD = 8
NEAR = tuple((dx, dy) for dx in (-1, 0, 1) for dy in (-1, 0, 1))

NT = (((1,), (1,)), ((), ()))
NN = (((1,), (0,)), ((), ()))


def iota(shape, dim):
    return lax.broadcasted_iota(I32, shape, dim)


def turn(v, by):
    return pltpu.roll(v, by % TX, 1)


def level(z):
    return pl.ds(pl.multiple_of(z * TY, TY), TY)


def cat(parts):
    return jnp.concatenate(parts, axis=0)


def dot(a, b, dims=NT):
    return lax.dot_general(a, b, dims, preferred_element_type=F32)


def split(v, count):
    parts = []
    for _ in range(count - 1):
        parts.append(v.astype(BF16).astype(F32))
        v = v - parts[-1]
    return [*parts, v]


def all_start(copies):
    for copy in copies:
        copy.start()


def all_wait(copies):
    for copy in copies:
        copy.wait()


def is_even(axis):
    return lax.rem(lax.axis_index(axis), 2) == 0


def records_kernel(
    rows_hbm, tile_hbm, cell_hbm, out_ref, rows_ref, tile_ref, cell_ref, parts, shifted, sems
):
    pairs = ((tile_hbm, tile_ref), (rows_hbm, rows_ref), (cell_hbm, cell_ref))
    coming = [pltpu.make_async_copy(hbm, ref, sems.at[n]) for n, (hbm, ref) in enumerate(pairs)]
    all_start(coming)
    shifted[...] = jnp.zeros(shifted.shape, F32)
    count = rows_ref.shape[1]
    devices = out_ref.shape[0] // 3
    all_wait(coming)
    named = (iota((devices, count), 0) == tile_ref[...]).astype(F32)
    earlier = (iota((count, count), 0) < iota((count, count), 1)).astype(F32).astype(BF16)
    picks = named.astype(BF16)
    before = dot(picks, earlier, NN)
    rank = jnp.sum(before * named, axis=0, keepdims=True).astype(I32)
    values = rows_ref[...]
    cells = (cell_ref[...] + 1).astype(F32)
    blocks = [jnp.where(rank == k, values, 0.0) for k in range(CAP)]
    blocks.append(jnp.where(rank == iota((8, count), 0), cells, 0.0))
    for k, block in enumerate(blocks):
        for n, part in enumerate(split(block, 3)):
            parts[n, 8 * k : 8 * k + 8, :] = part
    own = sum(dot(picks, parts[n].astype(BF16)) for n in range(3))
    shifted[32 : 32 + devices, 0:GROUP] = own
    lane = iota((devices, TX), 1)
    ty = lax.rem(iota((devices, TX), 0), 16)
    for c in range(3):
        chunk = jnp.zeros((devices, TX), F32)
        for i in range(3):
            dx, dy = NEAR[3 * c + i]
            off = 32 + 16 * dx + dy
            theirs = shifted[off : off + devices, :]
            held = (lane >= GROUP * i) & (lane < GROUP * (i + 1))
            if dy:
                held = held & (ty + dy >= 0) & (ty + dy < 16)
            chunk = jnp.where(held, turn(theirs, GROUP * i) if i else theirs, chunk)
        out_ref[pl.ds(c, devices, stride=3), :] = chunk


def edge_rows(out, t, a, f, high):
    edge = pl.ds(TY - 1 if high else 0, Z, stride=TY)
    inner = pl.ds(TY - 2 if high else 1, Z, stride=TY)
    out[0][...] = t[edge, :]
    out[1][...] = f[edge, :].astype(F32)
    out[2][...] = a[edge, :]
    out[3][...] = t[inner, :]
    up = (f[inner, :] & 2) != 0
    given = a[inner, :]
    out[4][...] = jnp.where(up, given, 0.0) if high else jnp.where(up, 0.0, given)


def by_parity(axis, first, second, fill):
    even = is_even(axis)

    @pl.when(even)
    def _():
        fill(first, True)
        fill(second, False)

    @pl.when(jnp.logical_not(even))
    def _():
        fill(first, False)
        fill(second, True)


def leaving_kernel(
    t_hbm, a_hbm, f_hbm,
    x0_ref, x1_ref, y0_ref, y1_ref, own_ref,
    t_ref, a_ref, f_ref, sems,
):
    arrays = ((t_hbm, t_ref), (a_hbm, a_ref), (f_hbm, f_ref))

    def copies(c):
        part = pl.ds(c * PART, PART)
        return [
            pltpu.make_async_copy(hbm.at[:, part, :], ref.at[:, part, :], sems.at[n, c])
            for n, (hbm, ref) in enumerate(arrays)
        ]

    for c in range(ROWS // PART):
        for copy in copies(c):
            copy.start()

    even = is_even("gx")
    lane = iota((TY, TX), 1)
    j = lane & 7

    def at_level(z, carry):
        here = level(z)
        packed = []
        for n, ref in enumerate((t_ref, a_ref, f_ref)):
            both = None
            for s in range(SRC):
                v = turn(ref[s, here, :].astype(F32), HALO + 8 * s)
                both = v if both is None else jnp.where(lane >> 3 == s, v, both)
            own_ref[n, here, :] = both
            packed.append(both)
        t, a, f = packed
        f = turn(f, 64)
        to_right = jnp.where(lane < 64, jnp.where(j < 4, t, turn(a, 4)), f)
        to_left = jnp.where(lane < 64, jnp.where(j < 4, turn(t, -4), a), f)
        x0_ref[here, :] = jnp.where(even, to_right, to_left)
        x1_ref[here, :] = jnp.where(even, to_left, to_right)
        return carry

    for c in range(ROWS // PART):
        for copy in copies(c):
            copy.wait()
        levels = PART // TY
        lax.fori_loop(c * levels, (c + 1) * levels, at_level, 0, unroll=8)

    def rows(out, high):
        for p in range(SRC):
            edge_rows([out.at[k, p] for k in range(5)], t_ref.at[p], a_ref.at[p], f_ref.at[p], high)

    by_parity("gy", y0_ref, y1_ref, rows)


def strips_kernel(
    own_ref, x0_ref, x1_ref, strip_out, y0_ref, y1_ref, strip_ref, f_ref, sems
):
    even = is_even("gx")
    shape = (ROWS, TX)
    lane = iota(shape, 1)
    near = (lane & 7) < 4
    low = lane < 64
    x0, x1 = x0_ref[...], x1_ref[...]
    left = jnp.where(even, x1, x0)
    right = jnp.where(even, x0, x1)
    t, a, f = own_ref[0], own_ref[1], own_ref[2]
    strip_ref[0] = jnp.where(
        low, jnp.where(near, left, t), turn(jnp.where(near, t, turn(right, 4)), 64)
    )
    strip_ref[1] = jnp.where(
        low, jnp.where(near, turn(left, -4), a), turn(jnp.where(near, a, right), 64)
    )
    flags = jnp.where(low, jnp.where(near, turn(left, 64), f), jnp.where(near, turn(f, 64), right))
    strip_ref[2] = flags
    f_ref[...] = flags.astype(I32)
    going = pltpu.make_async_copy(strip_ref, strip_out, sems.at[0])
    going.start()

    def rows(out, high):
        edge_rows([out.at[k] for k in range(5)], strip_ref.at[0], strip_ref.at[1], f_ref, high)

    by_parity("gy", y0_ref, y1_ref, rows)
    going.wait()


def both_sides(strip):
    return jnp.where((iota(strip.shape, 1) & 7) == 3, strip, turn(strip, 62))


def beside(v, patch, lane):
    if patch is None:
        return turn(v, 1), turn(v, -1)
    return jnp.where(lane == 0, patch, turn(v, 1)), jnp.where(lane == TX - 1, patch, turn(v, -1))


def patch_of(sides, p):
    return None if p == SRC else turn(sides, -(8 * p + 3))


def given_low(flag, bit, theirs, mine):
    return jnp.where((flag & bit) != 0, jnp.maximum(theirs - mine, 0.0), 0.0)


def given_high(flag, bit, theirs, mine):
    return jnp.where((flag & bit) == 0, jnp.maximum(theirs - mine, 0.0), 0.0)


def coef(flag, bit, low, high, mine):
    return jnp.maximum(mine - jnp.where((flag & bit) != 0, high, low), 0.0)


def take_rows(first, second, rows, flags, p, k):
    even = is_even("gy")
    here = pl.ds(PAD, Z)
    for side in range(2):
        v = jnp.where(even, second, first) if side == 0 else jnp.where(even, first, second)
        if k == 1:
            flags[side, p, here, :] = v.astype(I32)
        else:
            rows[side, k, p, here, :] = v


def shares_at(z, p, refs, sides, rows, flags, lane, row):
    t_p, a_p, f_p = refs
    here = level(z)
    below = level(jnp.maximum(z - 1, 0))
    above = level(jnp.minimum(z + 1, Z - 1))

    def halo(ref, *index):
        return jnp.broadcast_to(ref[(*index, pl.ds(PAD + z, 1), slice(None))], (TY, TX))

    def down(v, h):
        return jnp.where(row == 0, h, pltpu.roll(v, 1, 0))

    def up(v, h):
        return jnp.where(row == TY - 1, h, pltpu.roll(v, TY - 1, 0))

    t, f, a = t_p[here, :], f_p[here, :], a_p[here, :]
    tl, tr = beside(t, sides[0], lane)
    al, ar = beside(a, sides[1], lane)
    fl, fr = beside(f, sides[2], lane)
    tu, td = down(t, halo(rows, 0, 0, p)), up(t, halo(rows, 1, 0, p))
    fu, fd = down(f, halo(flags, 0, p)), up(f, halo(flags, 1, p))
    au, ad = down(a, halo(rows, 0, 2, p)), up(a, halo(rows, 1, 2, p))
    tm = jnp.where(z > 0, t_p[below, :], 0.0)
    tp = jnp.where(z < Z - 1, t_p[above, :], 0.0)
    den = 1.0 + coef(f, 1, tl, tr, t) + coef(f, 2, tu, td, t) + coef(f, 4, tm, tp, t)
    rden = 1.0 / den
    shares = [
        given_low(fl, 1, tl, t),
        given_high(fr, 1, tr, t),
        given_low(fu, 2, tu, t),
        given_high(fd, 2, td, t),
        given_low(f_p[below, :], 4, tm, t),
        given_high(f_p[above, :], 4, tp, t),
    ]
    shares = [g * rden for g in shares]
    total = None
    for g, v in zip(shares, (al, ar, au, ad, a_p[below, :], a_p[above, :])):
        total = g * v if total is None else total + g * v
    return shares, rden, total


def ones(mask):
    return jnp.where(mask, 1.0, 0.0).astype(BF16)


def scatter(rec_ref, main_ref, strip_ref, row_ref, turned, hot, levels, near, wide, main, columns):
    for c in range(3):
        turned[c] = rec_ref[pl.ds(c, TX, stride=3), :].T

    def held(dx, dy):
        g = NEAR.index((dx, dy))
        base = GROUP * (g % 3)
        values = [turned[g // 3, base + 8 * k : base + 8 * k + 8, :] for k in range(CAP)]
        return values, turned[g // 3, base + 32 : base + 40, :].astype(I32) - 1

    j = iota((TY, TX), 0)
    low16 = iota((16, TX), 0)
    deep = iota((Z, TX), 0)
    across = iota((TX, TX), 0)
    depth = CAP * TX
    for dy in (0, -1, 1):
        for n, dx in enumerate((-1, 0, 1)):
            values, cells = held(dx, dy)
            for k in range(CAP):
                cell = cells[k : k + 1, :]
                x = cell & (TX - 1)
                y = (cell >> 7) & (TY - 1)
                z = cell >> 10
                at = pl.ds(n * depth + k * TX, TX)
                if dy == 0:
                    for r in range(0, ROWS, 16):
                        hot[r : r + 16, at] = ones(low16 == (cell >> 7) - r)
                else:
                    z = jnp.where(y == (TY - 1 if dy < 0 else 0), z, -1)
                    levels[:, at] = ones(deep == z)
                parts = split(values[k], SPLIT)
                column = j == ((x + HALO) & (TX - 1))
                for side in range(2):
                    if dx == (1 if side == 0 else -1):
                        continue
                    inner = (dx == 0) == (side == 0)
                    use = column & ((j >= HALO) if inner else (j < HALO))
                    to = pl.ds((n - side) * depth + k * TX, TX)
                    for m in range(SPLIT):
                        for s in range(0, SRC, 2):
                            two = [jnp.where(use, parts[m][i : i + 1, :], 0.0) for i in (s, s + 1)]
                            near[side, m, 8 * s : 8 * s + 16, to] = cat(two).astype(BF16)
                if dx == 0:
                    to = pl.ds(k * TX, TX)
                    placed, spot, size = (main, x, TX) if dy == 0 else (wide, z, Z)
                    for r in range(0, size, 16):
                        mask = low16 == spot - r
                        for m in range(SPLIT):
                            for s in range(SRC):
                                one = jnp.where(mask, parts[m][s : s + 1, :], 0.0)
                                rows16 = slice(s * size + r, s * size + r + 16)
                                placed[m, rows16, to] = one.astype(BF16)
                    if dy:
                        columns[:, to] = ones(across == x)
        onehot = hot[...] if dy == 0 else levels[...]
        halves = []
        for side in range(2):
            some = onehot[:, side * depth : (side + 2) * depth]
            halves.append(sum(dot(some, near[side, m]) for m in range(SPLIT)))
        strip = jnp.concatenate(halves, axis=1)
        if dy == 0:
            strip_ref[...] = strip
            some = onehot[:, depth : 2 * depth]
            for s in range(0, SRC, 2):
                got = sum(dot(some, main[m, s * TX : (s + 2) * TX, :]) for m in range(SPLIT))
                main_ref[s] = got[:, :TX]
                main_ref[s + 1] = got[:, TX:]
        else:
            side = 0 if dy < 0 else 1
            row_ref[side, SRC] = strip
            got = sum(dot(wide[m], columns[...]) for m in range(SPLIT))
            for s in range(SRC):
                row_ref[side, s] = got[s * Z : (s + 1) * Z, :]


def core_kernel(
    rec_hbm, t_hbm, a_hbm, f_hbm, strip_hbm, y0_hbm, y1_hbm, h0_hbm, h1_hbm,
    last_ref, e0_ref, e1_ref, edge_ref, beyond_ref,
    rec_ref, t_ref, a_ref, f_ref, strip_in, y0_ref, y1_ref, h0_ref, h1_ref, strip_flags,
    turned, hot, levels, near, wide, main, columns, rows, flags, both, both_flags,
    g_ref, halo, back, adj, adj2, sems,
):
    pairs = (
        (rec_hbm, rec_ref),
        (y0_hbm, y0_ref),
        (y1_hbm, y1_ref),
        (strip_hbm, strip_in),
        (h0_hbm, h0_ref),
        (h1_hbm, h1_ref),
        (t_hbm, t_ref),
        (f_hbm, f_ref),
        (a_hbm, a_ref),
    )
    coming = [pltpu.make_async_copy(hbm, ref, sems.at[n]) for n, (hbm, ref) in enumerate(pairs)]
    all_start(coming)
    coming[0].wait()
    scatter(rec_ref, last_ref, last_ref.at[SRC], halo, turned, hot, levels, near, wide, main, columns)
    all_wait(coming[1:6])

    blank = jnp.zeros((PAD, TX), F32)
    for p in range(PLANES):
        for k in range(5):
            if p == SRC:
                take_rows(h0_ref[k], h1_ref[k], rows, flags, p, k)
            else:
                take_rows(y0_ref[k, p], y1_ref[k, p], rows, flags, p, k)
        for side in range(2):
            for k in (0, 2):
                rows[side, k, p, 0:PAD, :] = blank
                rows[side, k, p, PAD + Z : PAD + Z + PAD, :] = blank
    strip_flags[...] = strip_in[2].astype(I32)
    both[0] = both_sides(strip_in[0])
    both[1] = both_sides(strip_in[1])
    both_flags[...] = both_sides(strip_flags[...])
    lane = iota((TY, TX), 1)
    row = iota((TY, TX), 0)
    all_wait(coming[6:])

    def refs(p):
        if p < SRC:
            return t_ref.at[p], a_ref.at[p], f_ref.at[p]
        return strip_in.at[0], strip_in.at[1], strip_flags

    def at_level(z, carry):
        here = level(z)
        pair = [both[0, here, :], both[1, here, :], both_flags[here, :]]
        for p in range(PLANES):
            sides = [patch_of(v, p) for v in pair]
            shares, rden, total = shares_at(z, p, refs(p), sides, rows, flags, lane, row)
            for k, g in enumerate(shares):
                g_ref[k, p, here, :] = g
            source = last_ref[p, here, :] * rden
            last_ref[p, here, :] = source
            adj[p, here, :] = total + source
        return carry

    lax.fori_loop(0, Z, at_level, 0, unroll=4)

    wide_lane = iota((Z, TX), 1)
    for side in range(2):
        edge = pl.ds(0 if side == 0 else TY - 1, Z, stride=TY)
        here = pl.ds(PAD, Z)
        pair = [
            both_sides(rows[side, 0, SRC, here, :]),
            both_sides(rows[side, 2, SRC, here, :]),
            both_sides(flags[side, SRC, here, :]),
        ]
        for p in range(PLANES):
            t_p, a_p, f_p = refs(p)
            edge_ref[side, p] = g_ref[2 + side, p, edge, :]

            def at(k, shift=0):
                return rows[side, k, p, PAD + shift : PAD + shift + Z, :]

            t, a, f = at(0), at(2), flags[side, p, here, :]
            t2, a2 = at(3), at(4)
            t0, f0, a0 = t_p[edge, :], f_p[edge, :], a_p[edge, :]
            tl, tr = beside(t, patch_of(pair[0], p), wide_lane)
            al, ar = beside(a, patch_of(pair[1], p), wide_lane)
            fl, fr = beside(f, patch_of(pair[2], p), wide_lane)
            tm, tp = at(0, -1), at(0, 1)
            fm = flags[side, p, PAD - 1 : PAD - 1 + Z, :]
            fp = flags[side, p, PAD + 1 : PAD + 1 + Z, :]
            low, high = (t2, t0) if side == 0 else (t0, t2)
            den = 1.0 + coef(f, 1, tl, tr, t) + coef(f, 2, low, high, t) + coef(f, 4, tm, tp, t)
            rden = 1.0 / den
            inward = (given_high if side == 0 else given_low)(f0, 2, t0, t)
            total = halo[side, p] + given_low(fl, 1, tl, t) * al
            total = total + given_high(fr, 1, tr, t) * ar
            total = total + given_low(fm, 4, tm, t) * at(2, -1)
            total = total + given_high(fp, 4, tp, t) * at(2, 1)
            total = total + jnp.maximum(t2 - t, 0.0) * a2 + inward * a0
            halo[side, p] = total * rden
            back[side, p] = inward * rden

    def sweep(old, new, with_halo):
        both[0] = both_sides(old[SRC])

        def at_level(z, carry):
            here = level(z)
            below = level(jnp.maximum(z - 1, 0))
            above = level(jnp.minimum(z + 1, Z - 1))
            sides = both[0, here, :]
            for p in range(PLANES):
                v = old[p, here, :]
                left, right = beside(v, patch_of(sides, p), lane)
                low, high = 0.0, 0.0
                if with_halo:
                    low = jnp.broadcast_to(halo[0, p, pl.ds(z, 1), :], (TY, TX))
                    high = jnp.broadcast_to(halo[1, p, pl.ds(z, 1), :], (TY, TX))
                down = jnp.where(row == 0, low, pltpu.roll(v, 1, 0))
                up = jnp.where(row == TY - 1, high, pltpu.roll(v, TY - 1, 0))
                total = last_ref[p, here, :]
                for k, w in enumerate((left, right, down, up, old[p, below, :], old[p, above, :])):
                    total = total + g_ref[k, p, here, :] * w
                new[p, here, :] = total
            return carry

        lax.fori_loop(0, Z, at_level, 0, unroll=8)

    sweep(adj, adj2, True)
    sweep(adj2, last_ref, False)

    low, high = pl.ds(0, Z, stride=TY), pl.ds(TY - 1, Z, stride=TY)

    def pack(out, up):
        edge = high if up else low
        total = None
        for p in range(PLANES):
            out[p] = adj2[p, edge, :]
            if p < SRC:
                part = last_ref[p, edge, :]
                total = part if total is None else total + part
        out[PLANES] = total

    by_parity("gy", e0_ref, e1_ref, pack)
    for side, edge in enumerate((low, high)):
        total = None
        for s in range(SRC):
            part = back[side, s] * adj2[s, edge, :]
            total = part if total is None else total + part
        beyond_ref[side] = total


def gradient_kernel(
    last_hbm, slow_hbm, y0_ref, y1_ref, edge_ref, beyond_ref, adj_out, grad_out,
    last_ref, slow_ref, adj_ref, grad_ref, fix, above, patch, sums, in_sems, out_sems,
):
    parts = ROWS // PART

    def coming(c):
        part = pl.ds(c * PART, PART)
        return pltpu.make_async_copy(
            last_hbm.at[0:SRC, part, :], last_ref.at[0:SRC, part, :], in_sems.at[c]
        )

    def going(c):
        part = pl.ds(c * PART, PART)
        return pltpu.make_async_copy(adj_ref.at[:, part, :], adj_out.at[:, part, :], out_sems.at[c])

    strip_copy = pltpu.make_async_copy(last_hbm.at[SRC], last_ref.at[SRC], in_sems.at[parts])
    slow_copy = pltpu.make_async_copy(slow_hbm, slow_ref, in_sems.at[parts + 1])
    all_start([*(coming(c) for c in range(parts)), strip_copy, slow_copy])
    even_y = is_even("gy")
    for p in range(PLANES + 1):
        first, second = y0_ref[p], y1_ref[p]
        from_low = jnp.where(even_y, second, first)
        from_high = jnp.where(even_y, first, second)
        if p < PLANES:
            fix[0, p] = edge_ref[0, p] * from_low
            fix[1, p] = edge_ref[1, p] * from_high
        else:
            above[0] = beyond_ref[0] + from_low
            above[1] = beyond_ref[1] + from_high
    lane = iota((TY, TX), 1)
    row = iota((TY, TX), 0)

    def wide(ref, z, *index):
        return jnp.broadcast_to(ref[(*index, pl.ds(z, 1), slice(None))], (TY, TX))

    def completed(z, p):
        low, high = wide(fix, z, 0, p), wide(fix, z, 1, p)
        return last_ref[p, level(z), :] + jnp.where(
            row == 0, low, jnp.where(row == TY - 1, high, 0.0)
        )

    def own_level(z, carry):
        here = level(z)
        total = None
        for p in range(SRC):
            v = completed(z, p)
            adj_ref[p, here, :] = v
            total = v if total is None else total + v
        sums[here, :] = total
        return carry

    def strip_level(z, carry):
        patch[level(z), :] = completed(z, SRC)
        return carry

    def last_level(z, carry):
        here = level(z)
        total = sums[here, :]
        left, right = beside(total, patch[here, :], lane)
        down = jnp.where(row == 0, wide(above, z, 0), pltpu.roll(total, 1, 0))
        up = jnp.where(row == TY - 1, wide(above, z, 1), pltpu.roll(total, TY - 1, 0))
        beside_it = right + left + up + down
        grad_ref[here, :] = slow_ref[here, :] * (total + 0.125 * (beside_it - 4.0 * total))
        return carry

    levels = PART // TY
    for c in range(parts):
        coming(c).wait()
        lax.fori_loop(c * levels, (c + 1) * levels, own_level, 0, unroll=4)
        going(c).start()
    strip_copy.wait()
    lax.fori_loop(0, Z, strip_level, 0, unroll=8)
    strip = patch[...]
    for by in (8, 16, 32):
        strip = strip + turn(strip, by)
    patch[...] = jnp.where(iota((ROWS, TX), 1) == 0, turn(strip, -59), turn(strip, 3))
    slow_copy.wait()
    lax.fori_loop(0, Z, last_level, 0, unroll=8)
    grad_copy = pltpu.make_async_copy(grad_ref, grad_out, out_sems.at[parts])
    grad_copy.start()
    for c in range(parts):
        going(c).wait()
    grad_copy.wait()


def f32(*shape):
    return jax.ShapeDtypeStruct(shape, F32)


def call(kernel, outs, scratch, flops, ins=(), outs_in=(), limit=20):
    vmem = pl.BlockSpec(memory_space=pltpu.VMEM)

    def run(*args):
        moved = sum(a.size * 4 for a in args)
        given = [pl.BlockSpec(memory_space=s) for s in ins]
        kept = [pl.BlockSpec(memory_space=s) for s in outs_in]
        return pl.pallas_call(
            kernel,
            out_shape=outs,
            in_specs=given + [vmem] * (len(args) - len(given)),
            out_specs=kept + [vmem] * (len(outs) - len(kept)),
            scratch_shapes=scratch,
            compiler_params=pltpu.CompilerParams(vmem_limit_bytes=int(limit * 2**20)),
            cost_estimate=pl.CostEstimate(flops=flops, bytes_accessed=moved, transcendentals=0),
        )(*args)

    return run


def swapped(v, axis, count, odd):
    pairs = [(i, i + 1) for i in range(odd, count - 1, 2)]
    return lax.ppermute(v, axis, [(a, b) for a, b in pairs] + [(b, a) for a, b in pairs])


def shards(traveltime, adjoint_start, upwind_flags, slowness, residual_rows, station_tile, station_cell):
    devices = lax.axis_size(("gx", "gy"))
    nx, ny = lax.axis_size("gx"), lax.axis_size("gy")
    count = residual_rows.shape[0]
    t, a, f = (v.reshape(SRC, ROWS, TX) for v in (traveltime, adjoint_start, upwind_flags))
    whole = (SRC, ROWS, TX)

    x_out0, x_out1, y_out0, y_out1, own = call(
        leaving_kernel,
        [
            f32(ROWS, TX),
            f32(ROWS, TX),
            f32(5, SRC, Z, TX),
            f32(5, SRC, Z, TX),
            f32(3, ROWS, TX),
        ],
        [
            pltpu.VMEM(whole, F32),
            pltpu.VMEM(whole, F32),
            pltpu.VMEM(whole, I32),
            pltpu.SemaphoreType.DMA((3, ROWS // PART)),
        ],
        10**6,
        ins=[pltpu.HBM] * 3,
        limit=LEAVING_LIMIT,
    )(t, a, f)
    x_in0 = swapped(x_out0, "gx", nx, 0)
    x_in1 = swapped(x_out1, "gx", nx, 1)
    y_in0 = swapped(y_out0, "gy", ny, 0)
    y_in1 = swapped(y_out1, "gy", ny, 1)
    (sent,) = call(
        records_kernel,
        [f32(devices * 3, TX)],
        [
            pltpu.VMEM((SRC, count), F32),
            pltpu.VMEM((1, count), I32),
            pltpu.VMEM((1, count), I32),
            pltpu.VMEM((3, GROUP, count), F32),
            pltpu.VMEM((devices + 64, TX), F32),
            pltpu.SemaphoreType.DMA((3,)),
        ],
        10**6,
        ins=[pltpu.HBM] * 3,
        limit=RECORDS_LIMIT,
    )(residual_rows.T, station_tile.reshape(1, count), station_cell.reshape(1, count))
    got = lax.all_to_all(sent.reshape(devices, 1, 3 * TX), ("gx", "gy"), 0, 0, tiled=True)
    got = got.reshape(devices * 3, TX)

    strip, h_out0, h_out1 = call(
        strips_kernel,
        [f32(3, ROWS, TX), f32(5, Z, TX), f32(5, Z, TX)],
        [
            pltpu.VMEM((3, ROWS, TX), F32),
            pltpu.VMEM((ROWS, TX), I32),
            pltpu.SemaphoreType.DMA((1,)),
        ],
        10**6,
        outs_in=[pltpu.HBM],
    )(own, x_in0, x_in1)
    h_in0 = swapped(h_out0, "gy", ny, 0)
    h_in1 = swapped(h_out1, "gy", ny, 1)

    depth = CAP * TX
    last, e_out0, e_out1, edges, beyond = call(
        core_kernel,
        [
            f32(PLANES, ROWS, TX),
            f32(PLANES + 1, Z, TX),
            f32(PLANES + 1, Z, TX),
            f32(2, PLANES, Z, TX),
            f32(2, Z, TX),
        ],
        [
            pltpu.VMEM((devices * 3, TX), F32),
            pltpu.VMEM(whole, F32),
            pltpu.VMEM(whole, F32),
            pltpu.VMEM(whole, I32),
            pltpu.VMEM((3, ROWS, TX), F32),
            pltpu.VMEM((5, SRC, Z, TX), F32),
            pltpu.VMEM((5, SRC, Z, TX), F32),
            pltpu.VMEM((5, Z, TX), F32),
            pltpu.VMEM((5, Z, TX), F32),
            pltpu.VMEM((ROWS, TX), I32),
            pltpu.VMEM((3, TX, TX), F32),
            pltpu.VMEM((ROWS, 3 * depth), BF16),
            pltpu.VMEM((Z, 3 * depth), BF16),
            pltpu.VMEM((2, SPLIT, SRC * 8, 2 * depth), BF16),
            pltpu.VMEM((SPLIT, SRC * Z, depth), BF16),
            pltpu.VMEM((SPLIT, SRC * TX, depth), BF16),
            pltpu.VMEM((TX, depth), BF16),
            pltpu.VMEM((2, 5, PLANES, Z + 2 * PAD, TX), F32),
            pltpu.VMEM((2, PLANES, Z + 2 * PAD, TX), I32),
            pltpu.VMEM((2, ROWS, TX), F32),
            pltpu.VMEM((ROWS, TX), I32),
            pltpu.VMEM((6, PLANES, ROWS, TX), F32),
            pltpu.VMEM((2, PLANES, Z, TX), F32),
            pltpu.VMEM((2, PLANES, Z, TX), F32),
            pltpu.VMEM((PLANES, ROWS, TX), F32),
            pltpu.VMEM((PLANES, ROWS, TX), F32),
            pltpu.SemaphoreType.DMA((9,)),
        ],
        10**8,
        ins=[pltpu.HBM] * 9,
        limit=CORE_LIMIT,
    )(got, t, a, f, strip, y_in0, y_in1, h_in0, h_in1)
    e_in0 = swapped(e_out0, "gy", ny, 0)
    e_in1 = swapped(e_out1, "gy", ny, 1)

    parts = ROWS // PART
    adjoint, gradient = call(
        gradient_kernel,
        [f32(*whole), f32(ROWS, TX)],
        [
            pltpu.VMEM((PLANES, ROWS, TX), F32),
            pltpu.VMEM((ROWS, TX), F32),
            pltpu.VMEM(whole, F32),
            pltpu.VMEM((ROWS, TX), F32),
            pltpu.VMEM((2, PLANES, Z, TX), F32),
            pltpu.VMEM((2, Z, TX), F32),
            pltpu.VMEM((ROWS, TX), F32),
            pltpu.VMEM((ROWS, TX), F32),
            pltpu.SemaphoreType.DMA((parts + 2,)),
            pltpu.SemaphoreType.DMA((parts + 1,)),
        ],
        10**6,
        ins=[pltpu.HBM] * 2,
        outs_in=[pltpu.HBM] * 2,
        limit=GRADIENT_LIMIT,
    )(last, slowness.reshape(ROWS, TX), e_in0, e_in1, edges, beyond)
    return adjoint.reshape(traveltime.shape), gradient.reshape(slowness.shape)


def solution(mesh):
    placed = (
        P(None, None, "gy", "gx"),
        P(None, None, "gy", "gx"),
        P(None, None, "gy", "gx"),
        P(None, "gy", "gx"),
        P(("gx", "gy"), None),
        P(("gx", "gy"), None),
        P(("gx", "gy")),
    )

    return jax.shard_map(
        shards,
        mesh=mesh,
        in_specs=placed,
        out_specs=(P(None, None, "gy", "gx"), P(None, "gy", "gx")),
        check_vma=False,
    )
```
